64 devices in a mesh: dp: 8 (over x, y, core), sp: 8 (over z).
Axes of the slice: x: 2, y: 2, z: 8, core: 2. Of those that a mesh axis runs over, the one named last changes fastest.
The devices are a block of a 4x4x8 slice.
Arguments:
- q: bfloat16 [256, 4, 256], P('dp'), parts along dimension 0
- k: bfloat16 [256, 8192, 1, 256], P('dp', 'sp'), parts along dimension 0
- v: bfloat16 [256, 8192, 1, 256], P('dp', 'sp'), parts along dimension 0
Outputs:
- q: bfloat16 [256, 4, 256], P('dp'), parts along dimension 0
There are 8 independent parts. The reference program is written for one: setup_inputs(seed, part) draws one part's arguments, and reference() takes and returns one part's arrays. A program takes and returns all parts, laid end to end along the dimension named above; each array names one.
All inputs are finite; a program needn't handle non-finite values.
Results may differ from the reference program's by a relative error of at most 0.012.
Values are sent between devices in bfloat16 or wider.
A program may use at most 768 MiB of HBM per device.

```python
import jax
import jax.numpy as jnp

BATCH = 32
CACHE = 8192
HEADS = 4
KV_HEADS = 1
HEAD = 256


def setup_inputs(seed: int = 0, part: int = 0) -> dict:
    kq, kk, kv = (jax.random.fold_in(k, part) for k in jax.random.split(jax.random.key(seed), 3))
    return {
        "q": (3 * jax.random.normal(kq, (BATCH, HEADS, HEAD), jnp.float32)).astype(jnp.bfloat16),
        "k": jax.random.normal(kk, (BATCH, CACHE, KV_HEADS, HEAD), jnp.float32).astype(jnp.bfloat16),
        "v": jax.random.normal(kv, (BATCH, CACHE, KV_HEADS, HEAD), jnp.float32).astype(jnp.bfloat16),
    }


def einsum(form, a, b):
    return jnp.einsum(form, a.astype(jnp.float32), b.astype(jnp.float32))


def reference(q, k, v):
    grouped = q.reshape(BATCH, KV_HEADS, -1, HEAD)
    scores = einsum("bgsd,bugd->bgsu", grouped, k) * HEAD**-0.5
    weights = jax.nn.softmax(scores, -1).astype(jnp.bfloat16)
    return einsum("bgsu,bugd->bgsd", weights, v).astype(jnp.bfloat16).reshape(BATCH, HEADS, HEAD)
```

```python
import functools

import jax
import jax.numpy as jnp
from jax import lax
from jax.experimental import pallas as pl
from jax.experimental.pallas import tpu as pltpu
from jax.sharding import PartitionSpec as P

MESH = pl.DeviceIdType.MESH


def offset_of(step, n):
    return n // 2 + (step // 2 if step % 2 == 0 else -(step + 1) // 2)


def kernel(n, q_ref, k_hbm, v_hbm, o_ref, kbuf, vbuf, q_all, part, stat, part_in, stat_in, k_sem, v_sem, send_sem, recv_sem, out_send, out_recv):
    me = lax.axis_index("sp")
    sequences, heads, head = q_ref.shape
    each = sequences // n
    rows = each * heads
    owners = [lax.rem(me + offset_of(step, n), n) for step in range(n)]

    def fetch(step, j):
        at = owners[step] * each + j
        slot = step * each + j
        return (
            pltpu.make_async_copy(k_hbm.at[at], kbuf.at[slot], k_sem.at[slot]),
            pltpu.make_async_copy(v_hbm.at[at], vbuf.at[slot], v_sem.at[slot]),
        )

    for j in range(each):
        fetch(0, j)[0].start()
    for step in range(n):
        if step + 1 < n:
            for j in range(each):
                fetch(step + 1, j)[0].start()
        for j in range(each):
            fetch(step, j)[1].start()

    barrier = pltpu.get_barrier_semaphore()
    for d in range(1, n):
        pl.semaphore_signal(barrier, inc=1, device_id={"sp": lax.rem(me + d, n)}, device_id_type=MESH)

    for g in range(n):
        q_all[g] = jnp.concatenate([q_ref[g * each + j].astype(jnp.float32) for j in range(each)], 0).astype(jnp.bfloat16)

    row = lax.broadcasted_iota(jnp.int32, (rows, 1), 0) // heads
    lane = lax.broadcasted_iota(jnp.int32, (rows, 128), 1)

    def scores_of(step):
        q = q_all[owners[step]]
        scores = None
        for j in range(each):
            fetch(step, j)[0].wait()
            s = lax.dot_general(q, kbuf[step * each + j], (((1,), (1,)), ((), ())), preferred_element_type=jnp.float32)
            scores = s if scores is None else jnp.where(row == j, s, scores)
        return scores * head**-0.5

    def send(step):
        d = offset_of(step, n)
        peer = {"sp": owners[step]}
        return (
            pltpu.make_async_remote_copy(part.at[d], part_in.at[d], send_sem.at[d, 0], recv_sem.at[d, 0], device_id=peer, device_id_type=MESH),
            pltpu.make_async_remote_copy(stat.at[d], stat_in.at[d], send_sem.at[d, 1], recv_sem.at[d, 1], device_id=peer, device_id_type=MESH),
        )

    scores = scores_of(0)
    for step in range(n):
        following = scores_of(step + 1) if step + 1 < n else None
        high = jnp.max(scores, -1, keepdims=True)
        weights = jnp.exp(scores - high)
        total = jnp.sum(weights, -1, keepdims=True)
        weights = weights.astype(jnp.bfloat16)
        seen = None
        for j in range(each):
            fetch(step, j)[1].wait()
            s = jnp.dot(weights, vbuf[step * each + j], preferred_element_type=jnp.float32)
            seen = s if seen is None else jnp.where(row == j, s, seen)
        if step + 1 < n:
            d = offset_of(step, n)
            part[d] = seen.astype(jnp.bfloat16)
            stat[d] = jnp.where(lane < 64, total, high)
            if step == 0:
                pl.semaphore_wait(barrier, n - 1)
            for copy in send(step):
                copy.start()
        scores = following

    highs, totals = [high], [total]
    for d in range(1, n):
        for copy in send([offset_of(s, n) for s in range(n)].index(d)):
            copy.wait_recv()
        highs.append(stat_in[d][:, 64:65])
        totals.append(stat_in[d][:, 0:1])
    top = functools.reduce(jnp.maximum, highs)
    scales = [jnp.exp(h - top) for h in highs]
    whole = sum(t * s for t, s in zip(totals, scales))
    result = seen * scales[0]
    for d in range(1, n):
        result += part_in[d].astype(jnp.float32) * scales[d]
    o_ref[me] = (result / whole).astype(o_ref.dtype)

    def spread(d):
        return pltpu.make_async_remote_copy(
            o_ref.at[me], o_ref.at[me], out_send.at[d], out_recv.at[d], device_id={"sp": lax.rem(me + d, n)}, device_id_type=MESH
        )

    order = [offset_of(step, n) for step in range(n - 1)]
    for d in order:
        spread(d).start()
    for step in range(n - 1):
        for copy in send(step):
            copy.wait_send()
    for d in order:
        spread(d).wait_send()
    for d in order:
        source = lax.rem(me - d + n, n)
        pltpu.make_async_remote_copy(
            o_ref.at[source], o_ref.at[source], out_send.at[d], out_recv.at[d], device_id={"sp": lax.rem(me + d, n)}, device_id_type=MESH
        ).wait_recv()


def attend(n, q, k, v):
    sequences, heads, head = q.shape
    tokens = k.shape[1]
    rows = sequences // n * heads
    out = pl.pallas_call(
        functools.partial(kernel, n),
        out_shape=jax.ShapeDtypeStruct((n, rows, head), q.dtype),
        in_specs=[
            pl.BlockSpec(memory_space=pltpu.VMEM),
            pl.BlockSpec(memory_space=pl.ANY),
            pl.BlockSpec(memory_space=pl.ANY),
        ],
        out_specs=pl.BlockSpec(memory_space=pltpu.VMEM),
        scratch_shapes=[
            pltpu.VMEM((sequences, tokens, head), k.dtype),
            pltpu.VMEM((sequences, tokens, head), v.dtype),
            pltpu.VMEM((n, rows, head), q.dtype),
            pltpu.VMEM((n, rows, head), jnp.bfloat16),
            pltpu.VMEM((n, rows, 128), jnp.float32),
            pltpu.VMEM((n, rows, head), jnp.bfloat16),
            pltpu.VMEM((n, rows, 128), jnp.float32),
            pltpu.SemaphoreType.DMA((sequences,)),
            pltpu.SemaphoreType.DMA((sequences,)),
            pltpu.SemaphoreType.DMA((n, 2)),
            pltpu.SemaphoreType.DMA((n, 2)),
            pltpu.SemaphoreType.DMA((n,)),
            pltpu.SemaphoreType.DMA((n,)),
        ],
        compiler_params=pltpu.CompilerParams(collective_id=0, has_side_effects=True, vmem_limit_bytes=56 * 2**20),
    )(q, k.reshape(sequences, tokens, head), v.reshape(sequences, tokens, head))
    return out.reshape(q.shape)


def solution(mesh):
    return jax.shard_map(
        functools.partial(attend, mesh.shape["sp"]),
        mesh=mesh,
        in_specs=(P("dp", None, None), P("dp", "sp", None, None), P("dp", "sp", None, None)),
        out_specs=P("dp", None, None),
        check_vma=False,
    )
```

```python
import functools

import jax
import jax.numpy as jnp
from jax import lax
from jax.experimental import pallas as pl
from jax.experimental.pallas import tpu as pltpu
from jax.sharding import PartitionSpec as P

MESH = pl.DeviceIdType.MESH
TILE = 256
UNITS = 2


def offset_of(step, n):
    if isinstance(step, int):
        return n // 2 + (step // 2 if step % 2 == 0 else -(step + 1) // 2)
    return n // 2 + jnp.where(step % 2 == 0, step // 2, -((step + 1) // 2))


def kernel(n, q_ref, k_hbm, v_hbm, o_ref, *refs):
    sequences, heads, head = q_ref.shape
    each = sequences // n
    tiles = k_hbm.shape[1] // TILE
    deep = tiles // UNITS
    body(n, q_ref, k_hbm, v_hbm, o_ref, *refs, None)


def body(
    n, q_ref, k_hbm, v_hbm, o_ref, kbuf, vbuf, q_all, part, stat, part_in, stat_in, k_sem, v_sem, send_sem, recv_sem, out_send, out_recv, accs
):
    me = lax.axis_index("sp")
    sequences, heads, head = q_ref.shape
    each = sequences // n
    rows = each * heads
    tiles = kbuf.shape[1] // TILE
    deep = tiles // UNITS

    def owner(step):
        return lax.rem(me + offset_of(step, n), n)

    def fetch_k(step, j):
        slot = step * each + j
        return pltpu.make_async_copy(k_hbm.at[owner(step) * each + j], kbuf.at[slot], k_sem.at[slot])

    def fetch_v(step, j):
        slot = step * each + j
        return pltpu.make_async_copy(v_hbm.at[owner(step) * each + j], vbuf.at[slot], v_sem.at[slot])

    def start(fetch, step):
        for j in range(each):
            fetch(step, j).start()

    start(fetch_k, 0)

    @pl.loop(0, n - 1)
    def _(step):
        start(fetch_k, step + 1)
        start(fetch_v, step)

    start(fetch_v, n - 1)

    barrier = pltpu.get_barrier_semaphore()
    for d in range(1, n):
        pl.semaphore_signal(barrier, inc=1, device_id={"sp": lax.rem(me + d, n)}, device_id_type=MESH)

    for g in range(n):
        q_all[g] = jnp.concatenate([q_ref[g * each + j].astype(jnp.float32) for j in range(each)], 0).astype(jnp.bfloat16)

    row = lax.broadcasted_iota(jnp.int32, (rows, 1), 0) // heads
    lane = lax.broadcasted_iota(jnp.int32, (rows, 128), 1)

    def pick(values):
        out = values[0]
        for j in range(1, each):
            out = jnp.where(row == j, values[j], out)
        return out

    def multiply_k(step):
        q = q_all[owner(step)]
        out = {}
        for j in range(each):
            fetch_k(step, j).wait()
        for j in range(each):
            for t in range(deep):
                for u in range(UNITS):
                    at = (u * deep + t) * TILE
                    out[u, j, t] = lax.dot_general(
                        q, kbuf[step * each + j, at : at + TILE, :], (((1,), (1,)), ((), ())), preferred_element_type=jnp.float32
                    )
        return out

    def take_scores(out):
        return [
            pick([out[u, j, t] for j in range(each)]) * head**-0.5 for u in range(UNITS) for t in range(deep)
        ]

    def soften(scores):
        high = jnp.max(functools.reduce(jnp.maximum, scores), -1, keepdims=True)
        weights = [jnp.exp(s - high) for s in scores]
        total = jnp.sum(functools.reduce(jnp.add, weights), -1, keepdims=True)
        return high, total, [w.astype(jnp.bfloat16) for w in weights]

    def multiply_v(step, weights, split):
        out = {}
        if not split:
            for j in range(each):
                fetch_v(step, j).wait()
        for j in range(each):
            if split:
                fetch_v(step, j).wait()
            for t in range(deep):
                for u in range(UNITS):
                    at = (u * deep + t) * TILE
                    s = jnp.dot(weights[u * deep + t], vbuf[step * each + j, at : at + TILE, :], preferred_element_type=jnp.float32)
                    out[j] = out[j] + s if j in out else s
        return out

    def take_seen(out):
        return pick([out[j] for j in range(each)])

    def send(step):
        d = offset_of(step, n)
        peer = {"sp": owner(step)}
        return (
            pltpu.make_async_remote_copy(part.at[step], part_in.at[d], send_sem.at[step, 0], recv_sem.at[d, 0], device_id=peer, device_id_type=MESH),
            pltpu.make_async_remote_copy(stat.at[step], stat_in.at[d], send_sem.at[step, 1], recv_sem.at[d, 1], device_id=peer, device_id_type=MESH),
        )

    def turn(step, scores):
        out = multiply_k(step + 1)
        high, total, weights = soften(scores)
        seen = multiply_v(step, weights, False)
        following = take_scores(out)
        part[step] = take_seen(seen).astype(jnp.bfloat16)
        stat[step] = jnp.where(lane < 64, total, high)
        return following

    def dispatch(step):
        for copy in send(step):
            copy.start()

    scores = turn(0, take_scores(multiply_k(0)))
    pl.semaphore_wait(barrier, n - 1)
    dispatch(0)

    def loop(step, scores):
        scores = turn(step, scores)
        dispatch(step)
        return scores

    scores = lax.fori_loop(1, n - 1, loop, scores)
    high, total, weights = soften(scores)
    seen = take_seen(multiply_v(n - 1, weights, True))

    highs, totals = [high], [total]
    for step in range(n - 1):
        d = offset_of(step, n)
        for copy in send(step):
            copy.wait_recv()
        highs.append(stat_in[d][:, 64:65])
        totals.append(stat_in[d][:, 0:1])
    top = functools.reduce(jnp.maximum, highs)
    scales = [jnp.exp(h - top) for h in highs]
    whole = sum(t * s for t, s in zip(totals, scales))
    result = seen * scales[0]
    for step in range(n - 1):
        result += part_in[offset_of(step, n)].astype(jnp.float32) * scales[step + 1]
    o_ref[me] = (result / whole).astype(o_ref.dtype)

    def spread(d, block):
        return pltpu.make_async_remote_copy(
            o_ref.at[block], o_ref.at[block], out_send.at[d], out_recv.at[d], device_id={"sp": lax.rem(me + d, n)}, device_id_type=MESH
        )

    order = [offset_of(step, n) for step in range(n - 1)]
    for d in order:
        spread(d, me).start()
    for step in range(n - 1):
        for copy in send(step):
            copy.wait_send()
    for d in order:
        spread(d, me).wait_send()
    for d in order:
        spread(d, lax.rem(me - d + n, n)).wait_recv()


def attend(n, q, k, v):
    sequences, heads, head = q.shape
    tokens = k.shape[1]
    rows = sequences // n * heads
    out = pl.pallas_call(
        functools.partial(kernel, n),
        out_shape=jax.ShapeDtypeStruct((n, rows, head), q.dtype),
        in_specs=[
            pl.BlockSpec(memory_space=pltpu.VMEM),
            pl.BlockSpec(memory_space=pl.ANY),
            pl.BlockSpec(memory_space=pl.ANY),
        ],
        out_specs=pl.BlockSpec(memory_space=pltpu.VMEM),
        scratch_shapes=[
            pltpu.VMEM((sequences, tokens, head), k.dtype),
            pltpu.VMEM((sequences, tokens, head), v.dtype),
            pltpu.VMEM((n, rows, head), q.dtype),
            pltpu.VMEM((n, rows, head), jnp.bfloat16),
            pltpu.VMEM((n, rows, 128), jnp.float32),
            pltpu.VMEM((n, rows, head), jnp.bfloat16),
            pltpu.VMEM((n, rows, 128), jnp.float32),
            pltpu.SemaphoreType.DMA((sequences,)),
            pltpu.SemaphoreType.DMA((sequences,)),
            pltpu.SemaphoreType.DMA((n, 2)),
            pltpu.SemaphoreType.DMA((n, 2)),
            pltpu.SemaphoreType.DMA((n,)),
            pltpu.SemaphoreType.DMA((n,)),
        ],
        compiler_params=pltpu.CompilerParams(collective_id=0, has_side_effects=True, vmem_limit_bytes=56 * 2**20),
    )(q, k.reshape(sequences, tokens, head), v.reshape(sequences, tokens, head))
    return out.reshape(q.shape)


def solution(mesh):
    return jax.shard_map(
        functools.partial(attend, mesh.shape["sp"]),
        mesh=mesh,
        in_specs=(P("dp", None, None), P("dp", "sp", None, None), P("dp", "sp", None, None)),
        out_specs=P("dp", None, None),
        check_vma=False,
    )
```

```python
import functools

import jax
import jax.numpy as jnp
from jax import lax
from jax.experimental import pallas as pl
from jax.experimental.pallas import tpu as pltpu
from jax.sharding import PartitionSpec as P

MESH = pl.DeviceIdType.MESH
TILE = 256
AHEAD = 2


def offset_of(step, n):
    if isinstance(step, int):
        return n // 2 + (step // 2 if step % 2 == 0 else -(step + 1) // 2)
    return n // 2 + jnp.where(step % 2 == 0, step // 2, -((step + 1) // 2))


def kernel(
    n, q_hbm, k_hbm, v_hbm, o_ref, qbuf, kbuf, vbuf, q_all, s_all, w_all, sum_all, top_all, part, stat, part_in, stat_in,
    q_sem, k_sem, v_sem, last_sem, send_sem, recv_sem, out_send, out_recv,
):
    me = lax.axis_index("sp")
    sequences, heads, head = q_hbm.shape
    each = sequences // n
    rows = each * heads
    tiles = kbuf.shape[2] // TILE

    def owner(step):
        return lax.rem(me + offset_of(step, n), n)

    def run(step):
        return pl.ds(owner(step) * each, each)

    def fetch_k(step):
        return pltpu.make_async_copy(k_hbm.at[run(step)], kbuf.at[step], k_sem.at[step])

    def fetch_v(step):
        return pltpu.make_async_copy(v_hbm.at[run(step)], vbuf.at[step], v_sem.at[step])

    def fetch_last(j):
        return pltpu.make_async_copy(v_hbm.at[me * each + j], vbuf.at[n - 1, j], last_sem.at[j])

    def pieces(hbm, buf, sem, step):
        return [pltpu.make_async_copy(hbm.at[owner(step) * each + j], buf.at[step, j], sem.at[step]) for j in range(each)]

    def start_k(step):
        for piece in pieces(k_hbm, kbuf, k_sem, step):
            piece.start()

    def start_v(step):
        for piece in pieces(v_hbm, vbuf, v_sem, step):
            piece.start()

    fetch_q = pltpu.make_async_copy(q_hbm, qbuf, q_sem)
    start_k(0)
    fetch_q.start()

    for step in range(1, AHEAD):
        start_k(step)

    @pl.loop(0, n - AHEAD)
    def _(step):
        start_k(step + AHEAD)
        start_v(step)

    for step in range(n - AHEAD, n - 1):
        start_v(step)
    for j in range(each):
        fetch_last(j).start()

    barrier = pltpu.get_barrier_semaphore()
    for d in range(1, n):
        pl.semaphore_signal(barrier, inc=1, device_id={"sp": lax.rem(me + d, n)}, device_id_type=MESH)

    fetch_q.wait()
    for g in range(n):
        q_all[g] = jnp.concatenate([qbuf[g * each + j].astype(jnp.float32) for j in range(each)], 0).astype(jnp.bfloat16)

    row = lax.broadcasted_iota(jnp.int32, (rows, 1), 0) // heads
    lane = lax.broadcasted_iota(jnp.int32, (rows, 128), 1)

    def pick(values):
        out = values[0]
        for j in range(1, each):
            out = jnp.where(row == j, values[j], out)
        return out

    def span(t):
        return slice(t * TILE, (t + 1) * TILE)

    turns = [t + u * (tiles // 2) for t in range(tiles // 2) for u in range(2)]

    def score(step):
        q = q_all[owner(step)]
        out = {
            (j, t): lax.dot_general(q, kbuf[step, j, span(t), :], (((1,), (1,)), ((), ())), preferred_element_type=jnp.float32)
            for j in range(each)
            for t in turns
        }
        for t in range(tiles):
            s_all[step, t] = pick([out[j, t] for j in range(each)])

    def soften(step):
        scores = [s_all[step, t] * head**-0.5 for t in range(tiles)]
        high = jnp.max(functools.reduce(jnp.maximum, scores), -1, keepdims=True)
        weights = [jnp.exp(s - high) for s in scores]
        total = jnp.sum(functools.reduce(jnp.add, weights), -1, keepdims=True)
        for t in range(tiles):
            w_all[step, t] = weights[t].astype(jnp.bfloat16)
        stat[step] = jnp.where(lane < 64, total, high)

    def gather(step, split):
        out = []
        for j in range(each):
            if split:
                fetch_last(j).wait()
            dots = {t: jnp.dot(w_all[step, t], vbuf[step, j, span(t), :], preferred_element_type=jnp.float32) for t in turns}
            halves = [functools.reduce(jnp.add, [dots[t + u * (tiles // 2)] for t in range(tiles // 2)]) for u in range(2)]
            out.append(halves[0] + halves[1])
        return pick(out)

    def send(step):
        d = offset_of(step, n)
        peer = {"sp": owner(step)}
        return (
            pltpu.make_async_remote_copy(part.at[step], part_in.at[d], send_sem.at[step, 0], recv_sem.at[d, 0], device_id=peer, device_id_type=MESH),
            pltpu.make_async_remote_copy(stat.at[step], stat_in.at[d], send_sem.at[step, 1], recv_sem.at[d, 1], device_id=peer, device_id_type=MESH),
        )

    def dispatch(step):
        for copy in send(step):
            copy.start()

    @pl.loop(0, AHEAD)
    def _(step):
        fetch_k(step).wait()
        score(step)
        soften(step)

    @pl.loop(0, n - AHEAD)
    def _(step):
        fetch_k(step + AHEAD).wait()
        fetch_v(step).wait()
        score(step + AHEAD)
        part[step] = gather(step, False).astype(jnp.bfloat16)
        soften(step + AHEAD)

        @pl.when(step == 0)
        def _():
            pl.semaphore_wait(barrier, n - 1)

        dispatch(step)

    @pl.loop(n - AHEAD, n - 1)
    def _(step):
        fetch_v(step).wait()
        part[step] = gather(step, False).astype(jnp.bfloat16)
        dispatch(step)

    seen = gather(n - 1, True)
    high, total = stat[n - 1][:, 64:65], stat[n - 1][:, 0:1]

    def put(values):
        o_ref[me] = values.astype(o_ref.dtype)

    highs, totals = [high], [total]
    for step in range(n - 1):
        d = offset_of(step, n)
        for copy in send(step):
            copy.wait_recv()
        highs.append(stat_in[d][:, 64:65])
        totals.append(stat_in[d][:, 0:1])
    top = functools.reduce(jnp.maximum, highs)
    scales = [jnp.exp(h - top) for h in highs]
    whole = sum(t * s for t, s in zip(totals, scales))
    result = seen * scales[0]
    for step in range(n - 1):
        result += part_in[offset_of(step, n)].astype(jnp.float32) * scales[step + 1]
    put(result / whole)

    def spread(d, block):
        at = o_ref.at[block]
        return pltpu.make_async_remote_copy(
            at, at, out_send.at[d], out_recv.at[d], device_id={"sp": lax.rem(me + d, n)}, device_id_type=MESH
        )

    order = [offset_of(step, n) for step in range(n - 1)]
    for d in order:
        spread(d, me).start()
    for step in range(n - 1):
        for copy in send(step):
            copy.wait_send()
    for d in order:
        spread(d, me).wait_send()
    for d in order:
        spread(d, lax.rem(me - d + n, n)).wait_recv()


def attend(n, q, k, v):
    sequences, heads, head = q.shape
    tokens = k.shape[1]
    rows = sequences // n * heads
    tiles = tokens // TILE
    out = pl.pallas_call(
        functools.partial(kernel, n),
        out_shape=jax.ShapeDtypeStruct((n, rows, head), q.dtype),
        in_specs=[pl.BlockSpec(memory_space=pltpu.HBM)] * 3,
        out_specs=pl.BlockSpec(memory_space=pltpu.VMEM),
        scratch_shapes=[
            pltpu.VMEM(q.shape, q.dtype),
            pltpu.VMEM((n, sequences // n, tokens, head), k.dtype),
            pltpu.VMEM((n, sequences // n, tokens, head), v.dtype),
            pltpu.VMEM((n, rows, head), q.dtype),
            pltpu.VMEM((n, tiles, rows, TILE), jnp.float32),
            pltpu.VMEM((n, tiles, rows, TILE), jnp.bfloat16),
            pltpu.VMEM((n, rows, 128), jnp.float32),
            pltpu.VMEM((n, rows, 128), jnp.float32),
            pltpu.VMEM((n, rows, head), jnp.bfloat16),
            pltpu.VMEM((n, rows, 128), jnp.float32),
            pltpu.VMEM((n, rows, head), jnp.bfloat16),
            pltpu.VMEM((n, rows, 128), jnp.float32),
            pltpu.SemaphoreType.DMA,
            pltpu.SemaphoreType.DMA((n,)),
            pltpu.SemaphoreType.DMA((n,)),
            pltpu.SemaphoreType.DMA((sequences // n,)),
            pltpu.SemaphoreType.DMA((n, 2)),
            pltpu.SemaphoreType.DMA((n, 2)),
            pltpu.SemaphoreType.DMA((n,)),
            pltpu.SemaphoreType.DMA((n,)),
        ],
        compiler_params=pltpu.CompilerParams(collective_id=0, has_side_effects=True, vmem_limit_bytes=48 * 2**20),
    )(pltpu.with_memory_space_constraint(q, pltpu.HBM), k.reshape(sequences, tokens, head), v.reshape(sequences, tokens, head))
    return out.reshape(q.shape)


def solution(mesh):
    return jax.shard_map(
        functools.partial(attend, mesh.shape["sp"]),
        mesh=mesh,
        in_specs=(P("dp", None, None), P("dp", "sp", None, None), P("dp", "sp", None, None)),
        out_specs=P("dp", None, None),
        check_vma=False,
    )
```

```python
import functools

import jax
import jax.numpy as jnp
from jax import lax
from jax.experimental import pallas as pl
from jax.experimental.pallas import tpu as pltpu
from jax.sharding import PartitionSpec as P

MESH = pl.DeviceIdType.MESH
TILE = 256
AHEAD = 2


def offset_of(step, n):
    if isinstance(step, int):
        return n // 2 + step if step < n // 2 else n - 1 - step
    return jnp.where(step < n // 2, n // 2 + step, n - 1 - step)


def kernel(
    n, q_hbm, k_hbm, v_hbm, o_ref, qbuf, kbuf, vbuf, q_all, s_all, w_all, sum_all, top_all, part, stat, part_in, stat_in,
    q_sem, k_sem, v_sem, last_sem, send_sem, recv_sem, out_send, out_recv,
):
    me = lax.axis_index("sp")
    sequences, heads, head = q_hbm.shape
    each = sequences // n
    rows = each * heads
    tiles = kbuf.shape[2] // TILE

    def owner(step):
        return lax.rem(me + offset_of(step, n), n)

    def run(step):
        return pl.ds(owner(step) * each, each)

    def fetch_k(step):
        return pltpu.make_async_copy(k_hbm.at[run(step)], kbuf.at[step], k_sem.at[step])

    def fetch_v(step):
        return pltpu.make_async_copy(v_hbm.at[run(step)], vbuf.at[step], v_sem.at[step])

    def fetch_last(j):
        return pltpu.make_async_copy(v_hbm.at[me * each + j], vbuf.at[n - 1, j], last_sem.at[j])

    def pieces(hbm, buf, sem, step):
        return [pltpu.make_async_copy(hbm.at[owner(step) * each + j], buf.at[step, j], sem.at[step]) for j in range(each)]

    def start_k(step):
        for piece in pieces(k_hbm, kbuf, k_sem, step):
            piece.start()

    def start_v(step):
        for piece in pieces(v_hbm, vbuf, v_sem, step):
            piece.start()

    fetch_q = pltpu.make_async_copy(q_hbm, qbuf, q_sem)
    start_k(0)
    fetch_q.start()

    for step in range(1, AHEAD):
        start_k(step)

    @pl.loop(0, n - AHEAD)
    def _(step):
        start_k(step + AHEAD)
        start_v(step)

    for step in range(n - AHEAD, n - 1):
        start_v(step)
    for j in range(each):
        fetch_last(j).start()

    barrier = pltpu.get_barrier_semaphore()
    for d in range(1, n):
        pl.semaphore_signal(barrier, inc=1, device_id={"sp": lax.rem(me + d, n)}, device_id_type=MESH)

    fetch_q.wait()
    for g in range(n):
        q_all[g] = jnp.concatenate([qbuf[g * each + j].astype(jnp.float32) for j in range(each)], 0).astype(jnp.bfloat16)

    row = lax.broadcasted_iota(jnp.int32, (rows, 1), 0) // heads
    lane = lax.broadcasted_iota(jnp.int32, (rows, 128), 1)

    def pick(values):
        out = values[0]
        for j in range(1, each):
            out = jnp.where(row == j, values[j], out)
        return out

    def span(t):
        return slice(t * TILE, (t + 1) * TILE)

    turns = [t + u * (tiles // 2) for t in range(tiles // 2) for u in range(2)]

    def score(step):
        q = q_all[owner(step)]
        out = {
            (j, t): lax.dot_general(q, kbuf[step, j, span(t), :], (((1,), (1,)), ((), ())), preferred_element_type=jnp.float32)
            for j in range(each)
            for t in turns
        }
        for t in range(tiles):
            s_all[step, t] = pick([out[j, t] for j in range(each)])

    def soften(step):
        scores = [s_all[step, t] * head**-0.5 for t in range(tiles)]
        high = jnp.max(functools.reduce(jnp.maximum, scores), -1, keepdims=True)
        weights = [jnp.exp(s - high) for s in scores]
        total = jnp.sum(functools.reduce(jnp.add, weights), -1, keepdims=True)
        for t in range(tiles):
            w_all[step, t] = weights[t].astype(jnp.bfloat16)
        stat[step] = jnp.where(lane < 64, total, high)

    def gather(step, split):
        out = []
        for j in range(each):
            if split:
                fetch_last(j).wait()
            dots = {t: jnp.dot(w_all[step, t], vbuf[step, j, span(t), :], preferred_element_type=jnp.float32) for t in turns}
            halves = [functools.reduce(jnp.add, [dots[t + u * (tiles // 2)] for t in range(tiles // 2)]) for u in range(2)]
            out.append(halves[0] + halves[1])
        return pick(out)

    def send(step):
        d = offset_of(step, n)
        peer = {"sp": owner(step)}
        return (
            pltpu.make_async_remote_copy(part.at[step], part_in.at[d], send_sem.at[step, 0], recv_sem.at[d, 0], device_id=peer, device_id_type=MESH),
            pltpu.make_async_remote_copy(stat.at[step], stat_in.at[d], send_sem.at[step, 1], recv_sem.at[d, 1], device_id=peer, device_id_type=MESH),
        )

    def dispatch(step):
        for copy in send(step):
            copy.start()

    @pl.loop(0, AHEAD)
    def _(step):
        fetch_k(step).wait()
        score(step)
        soften(step)

    @pl.loop(0, n - AHEAD)
    def _(step):
        fetch_k(step + AHEAD).wait()
        fetch_v(step).wait()
        score(step + AHEAD)
        part[step] = gather(step, False).astype(jnp.bfloat16)
        soften(step + AHEAD)

        @pl.when(step == 0)
        def _():
            pl.semaphore_wait(barrier, n - 1)

        dispatch(step)

    @pl.loop(n - AHEAD, n - 1)
    def _(step):
        fetch_v(step).wait()
        part[step] = gather(step, False).astype(jnp.bfloat16)
        dispatch(step)

    seen = gather(n - 1, True)
    high, total = stat[n - 1][:, 64:65], stat[n - 1][:, 0:1]

    def put(values):
        o_ref[me] = values.astype(o_ref.dtype)

    highs, totals = [high], [total]
    for step in range(n - 1):
        d = offset_of(step, n)
        for copy in send(step):
            copy.wait_recv()
        highs.append(stat_in[d][:, 64:65])
        totals.append(stat_in[d][:, 0:1])
    top = functools.reduce(jnp.maximum, highs)
    scales = [jnp.exp(h - top) for h in highs]
    whole = sum(t * s for t, s in zip(totals, scales))
    result = seen * scales[0]
    for step in range(n - 1):
        result += part_in[offset_of(step, n)].astype(jnp.float32) * scales[step + 1]
    put(result / whole)

    def spread(d, block):
        at = o_ref.at[block]
        return pltpu.make_async_remote_copy(
            at, at, out_send.at[d], out_recv.at[d], device_id={"sp": lax.rem(me + d, n)}, device_id_type=MESH
        )

    order = [offset_of(step, n) for step in range(n - 1)]
    for d in order:
        spread(d, me).start()
    for step in range(n - 1):
        for copy in send(step):
            copy.wait_send()
    for d in order:
        spread(d, me).wait_send()
    for d in order:
        spread(d, lax.rem(me - d + n, n)).wait_recv()


def attend(n, q, k, v):
    sequences, heads, head = q.shape
    tokens = k.shape[1]
    rows = sequences // n * heads
    tiles = tokens // TILE
    out = pl.pallas_call(
        functools.partial(kernel, n),
        out_shape=jax.ShapeDtypeStruct((n, rows, head), q.dtype),
        in_specs=[pl.BlockSpec(memory_space=pltpu.HBM)] * 3,
        out_specs=pl.BlockSpec(memory_space=pltpu.VMEM),
        scratch_shapes=[
            pltpu.VMEM(q.shape, q.dtype),
            pltpu.VMEM((n, sequences // n, tokens, head), k.dtype),
            pltpu.VMEM((n, sequences // n, tokens, head), v.dtype),
            pltpu.VMEM((n, rows, head), q.dtype),
            pltpu.VMEM((n, tiles, rows, TILE), jnp.float32),
            pltpu.VMEM((n, tiles, rows, TILE), jnp.bfloat16),
            pltpu.VMEM((n, rows, 128), jnp.float32),
            pltpu.VMEM((n, rows, 128), jnp.float32),
            pltpu.VMEM((n, rows, head), jnp.bfloat16),
            pltpu.VMEM((n, rows, 128), jnp.float32),
            pltpu.VMEM((n, rows, head), jnp.bfloat16),
            pltpu.VMEM((n, rows, 128), jnp.float32),
            pltpu.SemaphoreType.DMA,
            pltpu.SemaphoreType.DMA((n,)),
            pltpu.SemaphoreType.DMA((n,)),
            pltpu.SemaphoreType.DMA((sequences // n,)),
            pltpu.SemaphoreType.DMA((n, 2)),
            pltpu.SemaphoreType.DMA((n, 2)),
            pltpu.SemaphoreType.DMA((n,)),
            pltpu.SemaphoreType.DMA((n,)),
        ],
        compiler_params=pltpu.CompilerParams(collective_id=0, has_side_effects=True, vmem_limit_bytes=48 * 2**20),
    )(pltpu.with_memory_space_constraint(q, pltpu.HBM), k.reshape(sequences, tokens, head), v.reshape(sequences, tokens, head))
    return out.reshape(q.shape)


def solution(mesh):
    return jax.shard_map(
        functools.partial(attend, mesh.shape["sp"]),
        mesh=mesh,
        in_specs=(P("dp", None, None), P("dp", "sp", None, None), P("dp", "sp", None, None)),
        out_specs=P("dp", None, None),
        check_vma=False,
    )
```

```python
import functools

import jax
import jax.numpy as jnp
from jax import lax
from jax.experimental import pallas as pl
from jax.experimental.pallas import tpu as pltpu
from jax.sharding import PartitionSpec as P

MESH = pl.DeviceIdType.MESH
TILE = 256
AHEAD = 2


def offset_of(step, n):
    if isinstance(step, int):
        return n // 2 + step if step < n // 2 else n - 1 - step
    return jnp.where(step < n // 2, n // 2 + step, n - 1 - step)


def kernel(
    n, q_hbm, k_hbm, v_hbm, o_ref, qbuf, kbuf, vbuf, q_all, s_all, w_all, sum_all, top_all, part, stat, part_in, stat_in,
    q_sem, k_sem, v_sem, send_sem, recv_sem, out_send, out_recv,
):
    me = lax.axis_index("sp")
    sequences, heads, head = q_hbm.shape
    each = sequences // n
    rows = each * heads
    tiles = kbuf.shape[2] // TILE

    def owner(step):
        return lax.rem(me + offset_of(step, n), n)

    def run(step):
        return pl.ds(owner(step) * each, each)

    def fetch_k(step):
        return pltpu.make_async_copy(k_hbm.at[run(step)], kbuf.at[step], k_sem.at[step])

    def fetch_v(step):
        return pltpu.make_async_copy(v_hbm.at[run(step)], vbuf.at[step], v_sem.at[step])

    def pieces(hbm, buf, sem, step):
        return [pltpu.make_async_copy(hbm.at[owner(step) * each + j], buf.at[step, j], sem.at[step]) for j in range(each)]

    def start_k(step):
        for piece in pieces(k_hbm, kbuf, k_sem, step):
            piece.start()

    def start_v(step):
        for piece in pieces(v_hbm, vbuf, v_sem, step):
            piece.start()

    fetch_q = pltpu.make_async_copy(q_hbm, qbuf, q_sem)
    start_k(0)
    fetch_q.start()

    for step in range(1, AHEAD):
        start_k(step)

    @pl.loop(0, n - AHEAD)
    def _(step):
        start_k(step + AHEAD)
        start_v(step)

    for step in range(n - AHEAD, n):
        start_v(step)

    barrier = pltpu.get_barrier_semaphore()
    for d in range(1, n):
        pl.semaphore_signal(barrier, inc=1, device_id={"sp": lax.rem(me + d, n)}, device_id_type=MESH)

    fetch_q.wait()
    for g in range(n):
        q_all[g] = jnp.concatenate([qbuf[g * each + j].astype(jnp.float32) for j in range(each)], 0).astype(jnp.bfloat16)

    row = lax.broadcasted_iota(jnp.int32, (rows, 1), 0) // heads
    lane = lax.broadcasted_iota(jnp.int32, (rows, 128), 1)

    def pick(values):
        out = values[0]
        for j in range(1, each):
            out = jnp.where(row == j, values[j], out)
        return out

    def span(t):
        return slice(t * TILE, (t + 1) * TILE)

    turns = [t + u * (tiles // 2) for t in range(tiles // 2) for u in range(2)]

    def score(step):
        q = q_all[owner(step)]
        out = {
            (j, t): lax.dot_general(q, kbuf[step, j, span(t), :], (((1,), (1,)), ((), ())), preferred_element_type=jnp.float32)
            for j in range(each)
            for t in turns
        }
        for t in range(tiles):
            s_all[step, t] = pick([out[j, t] for j in range(each)])

    def soften(step):
        scores = [s_all[step, t] * head**-0.5 for t in range(tiles)]
        high = jnp.max(functools.reduce(jnp.maximum, scores), -1, keepdims=True)
        weights = [jnp.exp(s - high) for s in scores]
        total = jnp.sum(functools.reduce(jnp.add, weights), -1, keepdims=True)
        for t in range(tiles):
            w_all[step, t] = weights[t].astype(jnp.bfloat16)
        stat[step] = jnp.where(lane < 64, total, high)

    def gather(step):
        out = []
        for j in range(each):
            dots = {t: jnp.dot(w_all[step, t], vbuf[step, j, span(t), :], preferred_element_type=jnp.float32) for t in turns}
            halves = [functools.reduce(jnp.add, [dots[t + u * (tiles // 2)] for t in range(tiles // 2)]) for u in range(2)]
            out.append(halves[0] + halves[1])
        return pick(out)

    def send(step):
        d = offset_of(step, n)
        peer = {"sp": owner(step)}
        return (
            pltpu.make_async_remote_copy(part.at[step], part_in.at[d], send_sem.at[step, 0], recv_sem.at[d, 0], device_id=peer, device_id_type=MESH),
            pltpu.make_async_remote_copy(stat.at[step], stat_in.at[d], send_sem.at[step, 1], recv_sem.at[d, 1], device_id=peer, device_id_type=MESH),
        )

    def dispatch(step):
        for copy in send(step):
            copy.start()

    @pl.loop(0, AHEAD)
    def _(step):
        fetch_k(step).wait()
        score(step)
        soften(step)

    @pl.loop(0, n - AHEAD)
    def _(step):
        fetch_k(step + AHEAD).wait()
        fetch_v(step).wait()
        score(step + AHEAD)
        part[step] = gather(step).astype(jnp.bfloat16)
        soften(step + AHEAD)

        @pl.when(step == 0)
        def _():
            pl.semaphore_wait(barrier, n - 1)

        dispatch(step)

    @pl.loop(n - AHEAD, n - 1)
    def _(step):
        fetch_v(step).wait()
        part[step] = gather(step).astype(jnp.bfloat16)
        dispatch(step)

    fetch_v(n - 1).wait()
    seen = gather(n - 1)
    high, total = stat[n - 1][:, 64:65], stat[n - 1][:, 0:1]

    def put(values):
        o_ref[me] = values.astype(o_ref.dtype)

    highs, totals = [high], [total]
    for step in range(n - 1):
        d = offset_of(step, n)
        for copy in send(step):
            copy.wait_recv()
        highs.append(stat_in[d][:, 64:65])
        totals.append(stat_in[d][:, 0:1])
    top = functools.reduce(jnp.maximum, highs)
    scales = [jnp.exp(h - top) for h in highs]
    whole = sum(t * s for t, s in zip(totals, scales))
    result = seen * scales[0]
    for step in range(n - 1):
        result += part_in[offset_of(step, n)].astype(jnp.float32) * scales[step + 1]
    put(result / whole)

    def spread(d, block):
        at = o_ref.at[block]
        return pltpu.make_async_remote_copy(
            at, at, out_send.at[d], out_recv.at[d], device_id={"sp": lax.rem(me + d, n)}, device_id_type=MESH
        )

    order = [offset_of(step, n) for step in range(n - 1)]
    for d in order:
        spread(d, me).start()
    for step in range(n - 1):
        for copy in send(step):
            copy.wait_send()
    for d in order:
        spread(d, me).wait_send()
    for d in order:
        spread(d, lax.rem(me - d + n, n)).wait_recv()


def attend(n, q, k, v):
    sequences, heads, head = q.shape
    tokens = k.shape[1]
    rows = sequences // n * heads
    tiles = tokens // TILE
    out = pl.pallas_call(
        functools.partial(kernel, n),
        out_shape=jax.ShapeDtypeStruct((n, rows, head), q.dtype),
        in_specs=[pl.BlockSpec(memory_space=pltpu.HBM)] * 3,
        out_specs=pl.BlockSpec(memory_space=pltpu.VMEM),
        scratch_shapes=[
            pltpu.VMEM(q.shape, q.dtype),
            pltpu.VMEM((n, sequences // n, tokens, head), k.dtype),
            pltpu.VMEM((n, sequences // n, tokens, head), v.dtype),
            pltpu.VMEM((n, rows, head), q.dtype),
            pltpu.VMEM((n, tiles, rows, TILE), jnp.float32),
            pltpu.VMEM((n, tiles, rows, TILE), jnp.bfloat16),
            pltpu.VMEM((n, rows, 128), jnp.float32),
            pltpu.VMEM((n, rows, 128), jnp.float32),
            pltpu.VMEM((n, rows, head), jnp.bfloat16),
            pltpu.VMEM((n, rows, 128), jnp.float32),
            pltpu.VMEM((n, rows, head), jnp.bfloat16),
            pltpu.VMEM((n, rows, 128), jnp.float32),
            pltpu.SemaphoreType.DMA,
            pltpu.SemaphoreType.DMA((n,)),
            pltpu.SemaphoreType.DMA((n,)),
            pltpu.SemaphoreType.DMA((n, 2)),
            pltpu.SemaphoreType.DMA((n, 2)),
            pltpu.SemaphoreType.DMA((n,)),
            pltpu.SemaphoreType.DMA((n,)),
        ],
        compiler_params=pltpu.CompilerParams(collective_id=0, has_side_effects=True, vmem_limit_bytes=48 * 2**20),
    )(pltpu.with_memory_space_constraint(q, pltpu.HBM), k.reshape(sequences, tokens, head), v.reshape(sequences, tokens, head))
    return out.reshape(q.shape)


def solution(mesh):
    return jax.shard_map(
        functools.partial(attend, mesh.shape["sp"]),
        mesh=mesh,
        in_specs=(P("dp", None, None), P("dp", "sp", None, None), P("dp", "sp", None, None)),
        out_specs=P("dp", None, None),
        check_vma=False,
    )
```

```python
import functools

import jax
import jax.numpy as jnp
from jax import lax
from jax.experimental import pallas as pl
from jax.experimental.pallas import tpu as pltpu
from jax.sharding import PartitionSpec as P

MESH = pl.DeviceIdType.MESH
TILE = 256
AHEAD = 2


def offset_of(step, n):
    order = sorted(range(n), key=lambda ahead: ahead if 2 * ahead < n else n - ahead + 1.5, reverse=True)
    if isinstance(step, int):
        return order[step]
    offset = order[0]
    for k in range(1, n):
        offset = jnp.where(step == k, order[k], offset)
    return offset


def kernel(
    n, q_hbm, k_hbm, v_hbm, o_ref, qbuf, kbuf, vbuf, q_all, s_all, w_all, sum_all, top_all, part, stat, part_in, stat_in,
    q_sem, k_sem, v_sem, send_sem, recv_sem, out_send, out_recv,
):
    me = lax.axis_index("sp")
    sequences, heads, head = q_hbm.shape
    each = sequences // n
    rows = each * heads
    tiles = kbuf.shape[2] // TILE

    def owner(step):
        return lax.rem(me + offset_of(step, n), n)

    def run(step):
        return pl.ds(owner(step) * each, each)

    def fetch_k(step):
        return pltpu.make_async_copy(k_hbm.at[run(step)], kbuf.at[step], k_sem.at[step])

    def fetch_v(step):
        return pltpu.make_async_copy(v_hbm.at[run(step)], vbuf.at[step], v_sem.at[step])

    def pieces(hbm, buf, sem, step):
        return [pltpu.make_async_copy(hbm.at[owner(step) * each + j], buf.at[step, j], sem.at[step]) for j in range(each)]

    def start_k(step):
        for piece in pieces(k_hbm, kbuf, k_sem, step):
            piece.start()

    def start_v(step):
        for piece in pieces(v_hbm, vbuf, v_sem, step):
            piece.start()

    fetch_q = pltpu.make_async_copy(q_hbm, qbuf, q_sem)
    start_k(0)
    fetch_q.start()

    for step in range(1, AHEAD):
        start_k(step)

    @pl.loop(0, n - AHEAD)
    def _(step):
        start_k(step + AHEAD)
        start_v(step)

    for step in range(n - AHEAD, n):
        start_v(step)

    barrier = pltpu.get_barrier_semaphore()
    for d in range(1, n):
        pl.semaphore_signal(barrier, inc=1, device_id={"sp": lax.rem(me + d, n)}, device_id_type=MESH)

    fetch_q.wait()
    for g in range(n):
        q_all[g] = jnp.concatenate([qbuf[g * each + j].astype(jnp.float32) for j in range(each)], 0).astype(jnp.bfloat16)

    row = lax.broadcasted_iota(jnp.int32, (rows, 1), 0) // heads
    lane = lax.broadcasted_iota(jnp.int32, (rows, 128), 1)

    def pick(values):
        out = values[0]
        for j in range(1, each):
            out = jnp.where(row == j, values[j], out)
        return out

    def span(t):
        return slice(t * TILE, (t + 1) * TILE)

    turns = [t + u * (tiles // 2) for t in range(tiles // 2) for u in range(2)]

    def score(step):
        q = q_all[owner(step)]
        out = {
            (j, t): lax.dot_general(q, kbuf[step, j, span(t), :], (((1,), (1,)), ((), ())), preferred_element_type=jnp.float32)
            for j in range(each)
            for t in turns
        }
        for t in range(tiles):
            s_all[step, t] = pick([out[j, t] for j in range(each)])

    def soften(step):
        scores = [s_all[step, t] * head**-0.5 for t in range(tiles)]
        high = jnp.max(functools.reduce(jnp.maximum, scores), -1, keepdims=True)
        weights = [jnp.exp(s - high) for s in scores]
        total = jnp.sum(functools.reduce(jnp.add, weights), -1, keepdims=True)
        for t in range(tiles):
            w_all[step, t] = weights[t].astype(jnp.bfloat16)
        stat[step] = jnp.where(lane < 64, total, high)

    def gather(step):
        out = []
        for j in range(each):
            dots = {t: jnp.dot(w_all[step, t], vbuf[step, j, span(t), :], preferred_element_type=jnp.float32) for t in turns}
            halves = [functools.reduce(jnp.add, [dots[t + u * (tiles // 2)] for t in range(tiles // 2)]) for u in range(2)]
            out.append(halves[0] + halves[1])
        return pick(out)

    def send(step):
        d = offset_of(step, n)
        peer = {"sp": owner(step)}
        return (
            pltpu.make_async_remote_copy(part.at[step], part_in.at[d], send_sem.at[step, 0], recv_sem.at[d, 0], device_id=peer, device_id_type=MESH),
            pltpu.make_async_remote_copy(stat.at[step], stat_in.at[d], send_sem.at[step, 1], recv_sem.at[d, 1], device_id=peer, device_id_type=MESH),
        )

    def dispatch(step):
        for copy in send(step):
            copy.start()

    @pl.loop(0, AHEAD)
    def _(step):
        fetch_k(step).wait()
        score(step)
        soften(step)

    @pl.loop(0, n - AHEAD)
    def _(step):
        fetch_k(step + AHEAD).wait()
        fetch_v(step).wait()
        score(step + AHEAD)
        part[step] = gather(step).astype(jnp.bfloat16)
        soften(step + AHEAD)

        @pl.when(step == 0)
        def _():
            pl.semaphore_wait(barrier, n - 1)

        dispatch(step)

    @pl.loop(n - AHEAD, n - 1)
    def _(step):
        fetch_v(step).wait()
        part[step] = gather(step).astype(jnp.bfloat16)
        dispatch(step)

    fetch_v(n - 1).wait()
    seen = gather(n - 1)
    high, total = stat[n - 1][:, 64:65], stat[n - 1][:, 0:1]

    def put(values):
        o_ref[me] = values.astype(o_ref.dtype)

    highs, totals = [high], [total]
    for step in range(n - 1):
        d = offset_of(step, n)
        for copy in send(step):
            copy.wait_recv()
        highs.append(stat_in[d][:, 64:65])
        totals.append(stat_in[d][:, 0:1])
    top = functools.reduce(jnp.maximum, highs)
    scales = [jnp.exp(h - top) for h in highs]
    whole = sum(t * s for t, s in zip(totals, scales))
    result = seen * scales[0]
    for step in range(n - 1):
        result += part_in[offset_of(step, n)].astype(jnp.float32) * scales[step + 1]
    put(result / whole)

    def spread(d, block):
        at = o_ref.at[block]
        return pltpu.make_async_remote_copy(
            at, at, out_send.at[d], out_recv.at[d], device_id={"sp": lax.rem(me + d, n)}, device_id_type=MESH
        )

    order = [offset_of(step, n) for step in range(n - 1)]
    for d in order:
        spread(d, me).start()
    for step in range(n - 1):
        for copy in send(step):
            copy.wait_send()
    for d in order:
        spread(d, me).wait_send()
    for d in order:
        spread(d, lax.rem(me - d + n, n)).wait_recv()


def attend(n, q, k, v):
    sequences, heads, head = q.shape
    tokens = k.shape[1]
    rows = sequences // n * heads
    tiles = tokens // TILE
    out = pl.pallas_call(
        functools.partial(kernel, n),
        out_shape=jax.ShapeDtypeStruct((n, rows, head), q.dtype),
        in_specs=[pl.BlockSpec(memory_space=pltpu.HBM)] * 3,
        out_specs=pl.BlockSpec(memory_space=pltpu.VMEM),
        scratch_shapes=[
            pltpu.VMEM(q.shape, q.dtype),
            pltpu.VMEM((n, sequences // n, tokens, head), k.dtype),
            pltpu.VMEM((n, sequences // n, tokens, head), v.dtype),
            pltpu.VMEM((n, rows, head), q.dtype),
            pltpu.VMEM((n, tiles, rows, TILE), jnp.float32),
            pltpu.VMEM((n, tiles, rows, TILE), jnp.bfloat16),
            pltpu.VMEM((n, rows, 128), jnp.float32),
            pltpu.VMEM((n, rows, 128), jnp.float32),
            pltpu.VMEM((n, rows, head), jnp.bfloat16),
            pltpu.VMEM((n, rows, 128), jnp.float32),
            pltpu.VMEM((n, rows, head), jnp.bfloat16),
            pltpu.VMEM((n, rows, 128), jnp.float32),
            pltpu.SemaphoreType.DMA,
            pltpu.SemaphoreType.DMA((n,)),
            pltpu.SemaphoreType.DMA((n,)),
            pltpu.SemaphoreType.DMA((n, 2)),
            pltpu.SemaphoreType.DMA((n, 2)),
            pltpu.SemaphoreType.DMA((n,)),
            pltpu.SemaphoreType.DMA((n,)),
        ],
        compiler_params=pltpu.CompilerParams(collective_id=0, has_side_effects=True, vmem_limit_bytes=48 * 2**20),
    )(pltpu.with_memory_space_constraint(q, pltpu.HBM), k.reshape(sequences, tokens, head), v.reshape(sequences, tokens, head))
    return out.reshape(q.shape)


def solution(mesh):
    return jax.shard_map(
        functools.partial(attend, mesh.shape["sp"]),
        mesh=mesh,
        in_specs=(P("dp", None, None), P("dp", "sp", None, None), P("dp", "sp", None, None)),
        out_specs=P("dp", None, None),
        check_vma=False,
    )
```
